32 devices in a mesh: groups: 2 (over y), freq: 16 (over z, x, core).
Axes of the slice: x: 2, y: 2, z: 4, core: 2. Of those that a mesh axis runs over, the one named last changes fastest.
Arguments:
- primary_one: bfloat16 [1024, 512, 512], P(('groups', 'freq')), parts along dimension 0, may hold values from -6 to 6
- primary_two: bfloat16 [1024, 512, 512], P(('groups', 'freq')), parts along dimension 0, may hold values from -6 to 6
- primary_three: bfloat16 [1024, 512, 512], P(('groups', 'freq')), parts along dimension 0, may hold values from -6 to 6
- window_start: int32 [3, 1024, 512], P(None, ('groups', 'freq')), parts along dimension 1, may hold values from 0 to 255
- window_end: int32 [3, 1024, 512], P(None, ('groups', 'freq')), parts along dimension 1, may hold values from 257 to 512
Outputs:
- predicted: bfloat16 [1024, 512, 512], P(('groups', 'freq')), parts along dimension 0
The draws below stay inside these ranges and needn't reach their ends.
There are 2 independent parts, one for each index of `groups`. The reference program is written for one: setup_inputs(seed, part) draws one part's arguments, and reference() takes and returns one part's arrays. A program takes and returns all parts, laid end to end along the dimension named above; each array names one. Nothing has to cross between parts.
Inputs may be any that keep to these rules, and one draw needn't show every extreme that they name: window_start of a trace is below its window_end.
All inputs are finite; a program needn't handle non-finite values.
Results may differ from the reference program's by a relative error of at most 0.0089.
Values may be sent and summed in bfloat16 or wider, within the bound.
A program may use at most 128 MiB of HBM per device.

```python
import jax
import jax.numpy as jnp
from jax import lax

NS = 512
NR = 512
NT = 512
NF = 16


def touch_ends(result, stream_key, least, high):
    index_at = [jax.random.randint(jax.random.fold_in(stream_key, axis), (), 0, length) for axis, length in enumerate(result.shape)]
    widest = result.shape.index(max(result.shape))
    beside = index_at[:widest] + [(index_at[widest] + 1) % result.shape[widest]] + index_at[widest + 1:]
    return result.at[tuple(index_at)].set(least).at[tuple(beside)].set(high)


def steps_of(stream_key, shape, cuts, low, largest):
    level = 1.0
    for dim, parts in cuts:
        steps = jax.random.uniform(jax.random.fold_in(jax.random.fold_in(stream_key, 6), dim), (parts,), jnp.float32, low / len(cuts), largest / len(cuts))
        level = level * jnp.repeat(jnp.exp(steps), shape[dim] // parts).reshape((-1,) + (1,) * (len(shape) - 1 - dim))
    return level


def centred(stream_key, shape, spread, reach, pieces=(), kind=jnp.bfloat16):
    gain = steps_of(stream_key, shape, pieces, -0.22, 0.18) if pieces else 1.0
    entries = jax.random.normal(stream_key, shape, jnp.float32) * spread * gain
    return jnp.minimum(jnp.maximum(entries, -reach), reach).astype(kind)


def setup_inputs(seed: int = 0, part: int = 0) -> dict:
    streams_of = jax.random.split(jax.random.key(seed), 6)
    part_splits = jax.random.split(jax.random.fold_in(streams_of[5], part), 6)
    return {
        "primary_one": centred(part_splits[0], (NS, NR, NT), 1.0, 6.0, ((0, 16),)),
        "primary_two": centred(part_splits[1], (NS, NR, NT), 1.0, 6.0, ((0, 16),)),
        "primary_three": centred(part_splits[2], (NS, NR, NT), 1.0, 6.0, ((0, 16),)),
        "window_start": touch_ends(jax.random.randint(part_splits[3], (3, NS, NR), 0, NT // 2), jax.random.fold_in(part_splits[3], 1), 0, (NT // 2) - 1).astype(jnp.int32),
        "window_end": touch_ends(jax.random.randint(part_splits[4], (3, NS, NR), NT // 2 + 1, NT + 1), jax.random.fold_in(part_splits[4], 1), NT // 2 + 1, NT).astype(jnp.int32),
    }


def make_table(count, samples):
    waves = jnp.arange(1, count + 1, dtype=jnp.int32)[:, None]
    times = jnp.arange(samples, dtype=jnp.int32)[None, :]
    phase = waves * times % samples
    angle = 2.0 * jnp.pi / samples * phase.astype(jnp.float32)
    both = jnp.stack([jnp.cos(angle), -jnp.sin(angle)], axis=1)
    return both.reshape(2 * count, samples).astype(jnp.bfloat16)

def spectrum(traces, start, finish, table):
    times = jnp.arange(NT, dtype=jnp.int32)
    inside = (times >= start[:, :, None]) & (times < finish[:, :, None])
    windowed = jnp.where(inside, traces, jnp.zeros_like(traces))
    flat = windowed.reshape(NS * NR, NT)
    spec = lax.dot_general(table, flat, (((1,), (1,)), ((), ())), preferred_element_type=jnp.float32)
    spec = spec * (1.0 / jnp.sqrt(jnp.float32(NT)))
    return spec.astype(jnp.bfloat16).reshape(NF, 2, NS, NR)

def slice_product(items):
    first, second, third = items
    first = first.astype(jnp.float32)
    second = second.astype(jnp.float32)
    third = third.astype(jnp.float32)
    high = lax.Precision.HIGHEST
    cross_re = jnp.dot(first[0], second[0].T, precision=high) + jnp.dot(first[1], second[1].T, precision=high)
    cross_im = jnp.dot(first[1], second[0].T, precision=high) - jnp.dot(first[0], second[1].T, precision=high)
    cross = (jnp.stack([cross_re, cross_im]) * (1.0 / jnp.sqrt(jnp.float32(NR)))).astype(jnp.bfloat16)
    cross = cross.astype(jnp.float32)
    mult_re = jnp.dot(cross[0], third[0], precision=high) - jnp.dot(cross[1], third[1], precision=high)
    mult_im = jnp.dot(cross[0], third[1], precision=high) + jnp.dot(cross[1], third[0], precision=high)
    return (jnp.stack([mult_re, mult_im]) * (1.0 / jnp.sqrt(jnp.float32(NS)))).astype(jnp.bfloat16)

def reference(primary_one, primary_two, primary_three, window_start, window_end):
    table = make_table(NF, NT)
    spec_one = spectrum(primary_one, window_start[0], window_end[0], table)
    spec_two = spectrum(primary_two, window_start[1], window_end[1], table)
    spec_three = spectrum(primary_three, window_start[2], window_end[2], table)
    multiple = lax.map(slice_product, (spec_one, spec_two, spec_three))
    flat = multiple.reshape(2 * NF, NS * NR)
    timed = lax.dot_general(flat, table, (((0,), (0,)), ((), ())), preferred_element_type=jnp.float32)
    timed = timed * (1.0 / jnp.sqrt(jnp.float32(NF)))
    return timed.astype(jnp.bfloat16).reshape(NS, NR, NT)
```

```python
import functools

import jax
import jax.numpy as jnp
from jax import lax
from jax.experimental import pallas as pl
from jax.experimental.pallas import tpu as pltpu
from jax.sharding import PartitionSpec as P

F_DEV = 1
GROUP = 16
LANES = 128


def make_table(count, samples):
    waves = jnp.arange(1, count + 1, dtype=jnp.int32)[:, None]
    times = jnp.arange(samples, dtype=jnp.int32)[None, :]
    phase = waves * times % samples
    angle = 2.0 * jnp.pi / samples * phase.astype(jnp.float32)
    both = jnp.stack([jnp.cos(angle), -jnp.sin(angle)], axis=1)
    return both.reshape(2 * count, samples).astype(jnp.bfloat16)


def exchange_kernel(
    n, sub, one_ref, two_ref, three_ref, start_ref, end_ref, table_ref, out_ref,
    buf, scr, stage, r1, r2, r3, gw, mbuf,
    load_sem, send_sem, r1_sem, r23_sem, out_sem,
):
    me = lax.axis_index("freq")
    sources, receivers, samples = one_ref.shape
    half = n // 2
    side = me // half
    quarter = n // 4
    rows_q = quarter * sources
    n_sub = GROUP // sub
    total = sources // sub

    def peer_far(q):
        return (1 - side) * half + lax.rem(me + q, half)

    def peer_near(q):
        return side * half + lax.rem(me + q, half)

    barrier = pltpu.get_barrier_semaphore()

    @pl.loop(1, n)
    def _(q):
        pl.semaphore_signal(
            barrier, inc=1, device_id={"freq": lax.rem(me + q, n)},
            device_id_type=pl.DeviceIdType.MESH,
        )

    sets = ((two_ref, 1, r2), (three_ref, 2, r3), (one_ref, 0, r1))

    def load(ref, i, slot):
        return pltpu.make_async_copy(
            ref.at[pl.ds(i * sub, sub)], buf.at[slot], load_sem.at[slot]
        )

    load(sets[0][0], 0, 0).start()
    scale_t = 1.0 / (samples ** 0.5)

    for k, (ref, which, landing) in enumerate(sets):
        if k < 2:
            arrive = r23_sem.at[k]
        else:
            arrive = r1_sem.at[me // quarter]

        @pl.loop(0, sources // GROUP)
        def _(g):
            @pl.loop(0, n_sub)
            def _(j):
                i = g * n_sub + j
                slot = lax.rem(i, 2)

                @pl.when(i + 1 < total)
                def _():
                    load(ref, i + 1, 1 - slot).start()

                if k < 2:
                    @pl.when(i + 1 == total)
                    def _():
                        load(sets[k + 1][0], 0, 0).start()

                load(ref, i, slot).wait()
                for s in range(sub):
                    row = i * sub + s
                    first = start_ref[which, pl.ds(row, 1), :]
                    last = end_ref[which, pl.ds(row, 1), :]
                    first = jnp.broadcast_to(first, (LANES, receivers)).T
                    last = jnp.broadcast_to(last, (LANES, receivers)).T
                    lane = lax.broadcasted_iota(jnp.int32, (receivers, LANES), 1)
                    pieces = []
                    for c in range(samples // LANES):
                        x = buf[slot, s, :, c * LANES:(c + 1) * LANES]
                        t = lane + c * LANES
                        keep = (t >= first) & (t < last)
                        pieces.append(jnp.where(keep, x, jnp.zeros_like(x)))
                    windowed = jnp.concatenate(pieces, axis=1)
                    spec = lax.dot_general(
                        table_ref[...], windowed, (((1,), (1,)), ((), ())),
                        preferred_element_type=jnp.float32,
                    )
                    scr[j * sub + s] = spec * scale_t

            at = pl.ds(pl.multiple_of(g * GROUP, GROUP), GROUP)
            for w in range(2 * n):
                stage[k, w // 2, w % 2, at, :] = scr[:, w, :].astype(jnp.bfloat16)

            if k == 0:
                @pl.when(g == 0)
                def _():
                    pl.semaphore_wait(barrier, n - 1)

                send_rows(k, g * GROUP, GROUP, landing, arrive, me, n, sources,
                          half, peer_far, peer_near, stage, send_sem)

        if k > 0:
            send_rows(k, 0, sources, landing, arrive, me, n, sources,
                      half, peer_far, peer_near, stage, send_sem)

    def drain(ref, sem):
        pltpu.make_async_copy(ref, ref, sem).wait()

    drain(r2, r23_sem.at[0])
    drain(r3, r23_sem.at[1])
    scale_g = 1.0 / ((n * sources) ** 0.5)
    scale_m = 1.0 / (receivers ** 0.5)
    width = 256

    @pl.loop(0, receivers // width)
    def _(b):
        cols = pl.ds(pl.multiple_of(b * width, width), width)
        ct = r2[0, :, cols].T
        dt = r2[1, :, cols].T
        e = r3[0]
        f = r3[1]
        dot = functools.partial(jnp.dot, preferred_element_type=jnp.float32)
        gw[cols, :receivers] = ((dot(ct, e) + dot(dt, f)) * scale_g).astype(jnp.bfloat16)
        gw[cols, receivers:] = ((dot(ct, f) - dot(dt, e)) * scale_g).astype(jnp.bfloat16)

    @pl.loop(0, 4)
    def _(step):
        other = (1 - side) * 2 + step
        own = side * 2 + lax.rem(step, 2)
        z = jnp.where(step < 2, other, own)
        rows = pl.ds(pl.multiple_of(z * rows_q, rows_q), rows_q)
        block = r1.at[:, rows, :]
        drain(block, r1_sem.at[z])
        both = jnp.concatenate([r1[0, rows, :], r1[1, rows, :]], axis=0)
        prod = jnp.dot(both, gw[...], preferred_element_type=jnp.float32)
        re = prod[:rows_q, :receivers] - prod[rows_q:, receivers:]
        im = prod[:rows_q, receivers:] + prod[rows_q:, :receivers]
        mbuf[0, rows, :] = (re * scale_m).astype(jnp.bfloat16)
        mbuf[1, rows, :] = (im * scale_m).astype(jnp.bfloat16)

        @pl.loop(0, quarter)
        def _(q):
            p = z * quarter + lax.rem(me + q, quarter)
            src = mbuf.at[:, pl.ds(pl.multiple_of(p * sources, sources), sources), :]

            @pl.when(p != me)
            def _():
                pltpu.make_async_remote_copy(
                    src_ref=src, dst_ref=out_ref.at[me],
                    send_sem=send_sem.at[3], recv_sem=out_sem,
                    device_id={"freq": p}, device_id_type=pl.DeviceIdType.MESH,
                ).start()

            @pl.when(p == me)
            def _():
                pltpu.make_async_copy(src, out_ref.at[me], out_sem).start()

    drain(out_ref, out_sem)
    for k in range(3):
        drain(stage.at[k, pl.ds(0, n - 1)], send_sem.at[k])
    drain(out_ref.at[pl.ds(0, n - 1)], send_sem.at[3])


def send_rows(k, base, count, landing, arrive, me, n, sources, half,
              peer_far, peer_near, stage, send_sem):
    if not isinstance(base, int):
        base = pl.multiple_of(base, GROUP)
    here = pl.ds(base, count)
    there = pl.ds(pl.multiple_of(me * sources + base, GROUP), count)

    def send(p):
        pltpu.make_async_remote_copy(
            src_ref=stage.at[k, p, :, here, :], dst_ref=landing.at[:, there, :],
            send_sem=send_sem.at[k], recv_sem=arrive,
            device_id={"freq": p}, device_id_type=pl.DeviceIdType.MESH,
        ).start()

    @pl.loop(0, half)
    def _(q):
        send(peer_far(q))

    @pl.loop(1, half)
    def _(q):
        send(peer_near(q))

    pltpu.make_async_copy(
        stage.at[k, me, :, here, :], landing.at[:, there, :], arrive
    ).start()


def spectrum(traces, start, finish, table, count):
    sources, receivers, samples = traces.shape
    times = jnp.arange(samples, dtype=jnp.int32)
    inside = (times >= start[:, :, None]) & (times < finish[:, :, None])
    windowed = jnp.where(inside, traces, jnp.zeros_like(traces))
    flat = windowed.reshape(sources * receivers, samples)
    spec = lax.dot_general(
        table, flat, (((1,), (1,)), ((), ())), preferred_element_type=jnp.float32
    )
    spec = spec * (1.0 / jnp.sqrt(jnp.float32(samples)))
    return spec.astype(jnp.bfloat16).reshape(count, 2, sources, receivers)


def correlate(first, second):
    swapped = jnp.stack([first[:, 1], -first[:, 0]], axis=1)
    left = jnp.stack([first, swapped], axis=1)
    cross = jnp.einsum("fkcsr,fcur->fksu", left, second, preferred_element_type=jnp.float32)
    cross = cross * (1.0 / jnp.sqrt(jnp.float32(first.shape[3])))
    return cross.astype(jnp.bfloat16)


def convolve(cross, third):
    right = jnp.stack(
        [
            jnp.stack([third[:, 0], -third[:, 1]], axis=1),
            jnp.stack([third[:, 1], third[:, 0]], axis=1),
        ],
        axis=1,
    )
    multiple = jnp.einsum("fcsu,fkcur->fksr", cross, right, preferred_element_type=jnp.float32)
    multiple = multiple * (1.0 / jnp.sqrt(jnp.float32(third.shape[2])))
    return multiple.astype(jnp.bfloat16)


def plain_on_device(primary_one, primary_two, primary_three, window_start, window_end):
    samples = primary_one.shape[2]
    count = F_DEV * lax.axis_size("freq")
    table = make_table(count, samples)
    spec_one = spectrum(primary_one, window_start[0], window_end[0], table, count)
    spec_two = spectrum(primary_two, window_start[1], window_end[1], table, count)
    spec_three = spectrum(primary_three, window_start[2], window_end[2], table, count)
    first, second, third = (
        lax.all_to_all(spec_one, "freq", split_axis=0, concat_axis=2, tiled=True),
        lax.all_to_all(spec_two, "freq", split_axis=0, concat_axis=2, tiled=True),
        lax.all_to_all(spec_three, "freq", split_axis=0, concat_axis=2, tiled=True),
    )
    cross = correlate(first, second)
    multiple = convolve(cross, third)
    piece = lax.all_to_all(multiple, "freq", split_axis=2, concat_axis=0, tiled=True)
    waves, parts, sources, receivers = piece.shape
    flat = piece.reshape(waves * parts, sources * receivers)
    timed = lax.dot_general(
        flat, table, (((0,), (0,)), ((), ())), preferred_element_type=jnp.float32
    )
    timed = timed * (1.0 / jnp.sqrt(jnp.float32(count)))
    return timed.astype(jnp.bfloat16).reshape(sources, receivers, samples)


def on_device(primary_one, primary_two, primary_three, window_start, window_end):
    sources, receivers, samples = primary_one.shape
    n = lax.axis_size("freq")
    if sources % GROUP or n % 4 or receivers % 256 or samples % LANES:
        return plain_on_device(
            primary_one, primary_two, primary_three, window_start, window_end
        )
    count = F_DEV * n
    table = make_table(count, samples)
    sub = max(1, min(GROUP // 2, (2 << 20) // (receivers * samples * 2)))
    bf = jnp.bfloat16
    whole = n * sources
    vmem = pl.BlockSpec(memory_space=pltpu.VMEM)
    hbm = pl.BlockSpec(memory_space=pl.ANY)
    piece = pl.pallas_call(
        functools.partial(exchange_kernel, n, sub),
        out_shape=jax.ShapeDtypeStruct((n, 2, sources, receivers), bf),
        in_specs=[hbm, hbm, hbm, vmem, vmem, vmem],
        out_specs=vmem,
        scratch_shapes=[
            pltpu.VMEM((2, sub, receivers, samples), bf),
            pltpu.VMEM((GROUP, 2 * count, receivers), jnp.float32),
            pltpu.VMEM((3, n, 2, sources, receivers), bf),
            pltpu.VMEM((2, whole, receivers), bf),
            pltpu.VMEM((2, whole, receivers), bf),
            pltpu.VMEM((2, whole, receivers), bf),
            pltpu.VMEM((receivers, 2 * receivers), bf),
            pltpu.VMEM((2, whole, receivers), bf),
            pltpu.SemaphoreType.DMA((2,)),
            pltpu.SemaphoreType.DMA((4,)),
            pltpu.SemaphoreType.DMA((4,)),
            pltpu.SemaphoreType.DMA((2,)),
            pltpu.SemaphoreType.DMA,
        ],
        compiler_params=pltpu.CompilerParams(
            collective_id=0, has_side_effects=True, vmem_limit_bytes=67000000,
        ),
        name="exchange",
    )(primary_one, primary_two, primary_three, window_start, window_end, table)
    flat = piece.reshape(2 * count, sources * receivers)
    timed = lax.dot_general(
        flat, table, (((0,), (0,)), ((), ())), preferred_element_type=jnp.float32
    )
    timed = timed * (1.0 / jnp.sqrt(jnp.float32(count)))
    return timed.astype(jnp.bfloat16).reshape(sources, receivers, samples)


def solution(mesh):
    return jax.shard_map(
        on_device,
        mesh=mesh,
        in_specs=(
            P(("groups", "freq"), None, None),
            P(("groups", "freq"), None, None),
            P(("groups", "freq"), None, None),
            P(None, ("groups", "freq"), None),
            P(None, ("groups", "freq"), None),
        ),
        out_specs=P(("groups", "freq"), None, None),
        check_vma=False,
    )
```

```python
import functools

import jax
import jax.numpy as jnp
from jax import lax
from jax.experimental import pallas as pl
from jax.experimental.pallas import tpu as pltpu
from jax.sharding import PartitionSpec as P

F_DEV = 1
GROUP = 16
LANES = 128


def make_table(count, samples):
    waves = jnp.arange(1, count + 1, dtype=jnp.int32)[:, None]
    times = jnp.arange(samples, dtype=jnp.int32)[None, :]
    phase = waves * times % samples
    angle = 2.0 * jnp.pi / samples * phase.astype(jnp.float32)
    both = jnp.stack([jnp.cos(angle), -jnp.sin(angle)], axis=1)
    return both.reshape(2 * count, samples).astype(jnp.bfloat16)


def exchange_kernel(
    n, sub, one_ref, two_ref, three_ref, start_ref, end_ref, table_ref, out_ref,
    buf, scr, stage, r1, r2, r3, gw, mbuf,
    load_sem, send_sem, r1_sem, r23_sem, out_sem,
):
    me = lax.axis_index("freq")
    sources, receivers, samples = one_ref.shape
    half = n // 2
    side = me // half
    n_sub = GROUP // sub
    total = sources // sub

    def peer_far(q):
        return (1 - side) * half + lax.rem(me + q, half)

    def peer_near(q):
        return side * half + lax.rem(me + q, half)

    barrier = pltpu.get_barrier_semaphore()

    @pl.loop(1, n)
    def _(q):
        pl.semaphore_signal(
            barrier, inc=1, device_id={"freq": lax.rem(me + q, n)},
            device_id_type=pl.DeviceIdType.MESH,
        )

    sets = ((two_ref, 1, r2), (three_ref, 2, r3), (one_ref, 0, r1))

    def load(ref, i, slot):
        return pltpu.make_async_copy(
            ref.at[pl.ds(i * sub, sub)], buf.at[slot], load_sem.at[slot]
        )

    load(sets[0][0], 0, 0).start()
    scale_t = 1.0 / (samples ** 0.5)

    for k, (ref, which, landing) in enumerate(sets):
        if k < 2:
            arrive = r23_sem.at[k]
        else:
            arrive = r1_sem.at[me]

        @pl.loop(0, sources // GROUP)
        def _(g):
            @pl.loop(0, n_sub)
            def _(j):
                i = g * n_sub + j
                slot = lax.rem(i, 2)

                @pl.when(i + 1 < total)
                def _():
                    load(ref, i + 1, 1 - slot).start()

                if k < 2:
                    @pl.when(i + 1 == total)
                    def _():
                        load(sets[k + 1][0], 0, 0).start()

                load(ref, i, slot).wait()
                for s in range(sub):
                    row = i * sub + s
                    packed = (
                        start_ref[which, pl.ds(row, 1), :] * 4096
                        + end_ref[which, pl.ds(row, 1), :]
                    )
                    packed = jnp.broadcast_to(packed, (LANES, receivers)).T
                    first = packed >> 12
                    last = packed & 4095
                    lane = lax.broadcasted_iota(jnp.int32, (receivers, LANES), 1)
                    pieces = []
                    for c in range(samples // LANES):
                        x = buf[slot, s, :, c * LANES:(c + 1) * LANES]
                        t = lane + c * LANES
                        keep = (t >= first) & (t < last)
                        pieces.append(jnp.where(keep, x, jnp.zeros_like(x)))
                    windowed = jnp.concatenate(pieces, axis=1)
                    spec = lax.dot_general(
                        table_ref[...], windowed, (((1,), (1,)), ((), ())),
                        preferred_element_type=jnp.float32,
                    )
                    scr[j * sub + s] = spec * scale_t

            at = pl.ds(pl.multiple_of(g * GROUP, GROUP), GROUP)
            for w in range(2 * n):
                stage[k, w // 2, w % 2, at, :] = scr[:, w, :].astype(jnp.bfloat16)

            if k == 0:
                @pl.when(g == 0)
                def _():
                    pl.semaphore_wait(barrier, n - 1)

                send_rows(k, g * GROUP, GROUP, landing, arrive, me, n, sources,
                          half, peer_far, peer_near, stage, send_sem)

        if k > 0:
            send_rows(k, 0, sources, landing, arrive, me, n, sources,
                      half, peer_far, peer_near, stage, send_sem)

    def drain(ref, sem):
        pltpu.make_async_copy(ref, ref, sem).wait()

    drain(r2, r23_sem.at[0])
    drain(r3, r23_sem.at[1])
    scale_g = 1.0 / ((n * sources) ** 0.5)
    scale_m = 1.0 / (receivers ** 0.5)
    width = 256

    @pl.loop(0, receivers // width)
    def _(b):
        cols = pl.ds(pl.multiple_of(b * width, width), width)
        ct = r2[0, :, cols].T
        dt = r2[1, :, cols].T
        e = r3[0]
        f = r3[1]
        dot = functools.partial(jnp.dot, preferred_element_type=jnp.float32)
        gw[cols, :receivers] = ((dot(ct, e) + dot(dt, f)) * scale_g).astype(jnp.bfloat16)
        gw[cols, receivers:] = ((dot(ct, f) - dot(dt, e)) * scale_g).astype(jnp.bfloat16)

    @pl.loop(0, n)
    def _(step):
        place = lax.rem(me + n - step, half)
        p = jnp.where(step < half, side, 1 - side) * half + place
        rows = pl.ds(pl.multiple_of(p * sources, sources), sources)
        drain(r1.at[:, rows, :], r1_sem.at[p])
        both = jnp.concatenate([r1[0, rows, :], r1[1, rows, :]], axis=0)
        prod = jnp.dot(both, gw[...], preferred_element_type=jnp.float32)
        re = prod[:sources, :receivers] - prod[sources:, receivers:]
        im = prod[:sources, receivers:] + prod[sources:, :receivers]
        mbuf[0, rows, :] = (re * scale_m).astype(jnp.bfloat16)
        mbuf[1, rows, :] = (im * scale_m).astype(jnp.bfloat16)
        src = mbuf.at[:, rows, :]

        @pl.when(p != me)
        def _():
            pltpu.make_async_remote_copy(
                src_ref=src, dst_ref=out_ref.at[me],
                send_sem=send_sem.at[3], recv_sem=out_sem,
                device_id={"freq": p}, device_id_type=pl.DeviceIdType.MESH,
            ).start()

        @pl.when(p == me)
        def _():
            pltpu.make_async_copy(src, out_ref.at[me], out_sem).start()

    drain(out_ref, out_sem)
    for k in range(3):
        drain(stage.at[k, pl.ds(0, n - 1)], send_sem.at[k])
    drain(out_ref.at[pl.ds(0, n - 1)], send_sem.at[3])


def send_rows(k, base, count, landing, arrive, me, n, sources, half,
              peer_far, peer_near, stage, send_sem):
    if not isinstance(base, int):
        base = pl.multiple_of(base, GROUP)
    here = pl.ds(base, count)
    there = pl.ds(pl.multiple_of(me * sources + base, GROUP), count)

    def send(p):
        pltpu.make_async_remote_copy(
            src_ref=stage.at[k, p, :, here, :], dst_ref=landing.at[:, there, :],
            send_sem=send_sem.at[k], recv_sem=arrive,
            device_id={"freq": p}, device_id_type=pl.DeviceIdType.MESH,
        ).start()

    def far():
        @pl.loop(0, half)
        def _(q):
            send(peer_far(q))

    def near():
        pltpu.make_async_copy(
            stage.at[k, me, :, here, :], landing.at[:, there, :], arrive
        ).start()

        @pl.loop(1, half)
        def _(q):
            send(peer_near(q))

    if k == 2:
        near()
        far()
    else:
        far()
        near()


def inverse_kernel(piece_ref, table_ref, out_ref, scr):
    count = piece_ref.shape[0]
    step = pl.program_id(0)
    sub = out_ref.shape[0]
    per = GROUP // sub

    @pl.when(lax.rem(step, per) == 0)
    def _():
        at = pl.ds(pl.multiple_of(step // per * GROUP, GROUP), GROUP)
        for w in range(2 * count):
            scr[:, w, :] = piece_ref[w // 2, w % 2, at, :].astype(jnp.float32)

    scale = 1.0 / (count ** 0.5)
    for s in range(sub):
        row = lax.rem(step, per) * sub + s
        timed = lax.dot_general(
            scr[row].astype(jnp.bfloat16), table_ref[...],
            (((0,), (0,)), ((), ())), preferred_element_type=jnp.float32,
        )
        out_ref[s] = (timed * scale).astype(jnp.bfloat16)


def spectrum(traces, start, finish, table, count):
    sources, receivers, samples = traces.shape
    times = jnp.arange(samples, dtype=jnp.int32)
    inside = (times >= start[:, :, None]) & (times < finish[:, :, None])
    windowed = jnp.where(inside, traces, jnp.zeros_like(traces))
    flat = windowed.reshape(sources * receivers, samples)
    spec = lax.dot_general(
        table, flat, (((1,), (1,)), ((), ())), preferred_element_type=jnp.float32
    )
    spec = spec * (1.0 / jnp.sqrt(jnp.float32(samples)))
    return spec.astype(jnp.bfloat16).reshape(count, 2, sources, receivers)


def correlate(first, second):
    swapped = jnp.stack([first[:, 1], -first[:, 0]], axis=1)
    left = jnp.stack([first, swapped], axis=1)
    cross = jnp.einsum("fkcsr,fcur->fksu", left, second, preferred_element_type=jnp.float32)
    cross = cross * (1.0 / jnp.sqrt(jnp.float32(first.shape[3])))
    return cross.astype(jnp.bfloat16)


def convolve(cross, third):
    right = jnp.stack(
        [
            jnp.stack([third[:, 0], -third[:, 1]], axis=1),
            jnp.stack([third[:, 1], third[:, 0]], axis=1),
        ],
        axis=1,
    )
    multiple = jnp.einsum("fcsu,fkcur->fksr", cross, right, preferred_element_type=jnp.float32)
    multiple = multiple * (1.0 / jnp.sqrt(jnp.float32(third.shape[2])))
    return multiple.astype(jnp.bfloat16)


def plain_on_device(primary_one, primary_two, primary_three, window_start, window_end):
    samples = primary_one.shape[2]
    count = F_DEV * lax.axis_size("freq")
    table = make_table(count, samples)
    spec_one = spectrum(primary_one, window_start[0], window_end[0], table, count)
    spec_two = spectrum(primary_two, window_start[1], window_end[1], table, count)
    spec_three = spectrum(primary_three, window_start[2], window_end[2], table, count)
    first, second, third = (
        lax.all_to_all(spec_one, "freq", split_axis=0, concat_axis=2, tiled=True),
        lax.all_to_all(spec_two, "freq", split_axis=0, concat_axis=2, tiled=True),
        lax.all_to_all(spec_three, "freq", split_axis=0, concat_axis=2, tiled=True),
    )
    cross = correlate(first, second)
    multiple = convolve(cross, third)
    piece = lax.all_to_all(multiple, "freq", split_axis=2, concat_axis=0, tiled=True)
    waves, parts, sources, receivers = piece.shape
    flat = piece.reshape(waves * parts, sources * receivers)
    timed = lax.dot_general(
        flat, table, (((0,), (0,)), ((), ())), preferred_element_type=jnp.float32
    )
    timed = timed * (1.0 / jnp.sqrt(jnp.float32(count)))
    return timed.astype(jnp.bfloat16).reshape(sources, receivers, samples)


def on_device(primary_one, primary_two, primary_three, window_start, window_end):
    sources, receivers, samples = primary_one.shape
    n = lax.axis_size("freq")
    if sources % GROUP or n % 2 or receivers % 256 or samples % LANES:
        return plain_on_device(
            primary_one, primary_two, primary_three, window_start, window_end
        )
    count = F_DEV * n
    table = make_table(count, samples)
    sub = max(1, min(GROUP // 2, (2 << 20) // (receivers * samples * 2)))
    bf = jnp.bfloat16
    whole = n * sources
    vmem = pl.BlockSpec(memory_space=pltpu.VMEM)
    hbm = pl.BlockSpec(memory_space=pl.ANY)
    piece = pl.pallas_call(
        functools.partial(exchange_kernel, n, sub),
        out_shape=jax.ShapeDtypeStruct((n, 2, sources, receivers), bf),
        in_specs=[hbm, hbm, hbm, vmem, vmem, vmem],
        out_specs=vmem,
        scratch_shapes=[
            pltpu.VMEM((2, sub, receivers, samples), bf),
            pltpu.VMEM((GROUP, 2 * count, receivers), jnp.float32),
            pltpu.VMEM((3, n, 2, sources, receivers), bf),
            pltpu.VMEM((2, whole, receivers), bf),
            pltpu.VMEM((2, whole, receivers), bf),
            pltpu.VMEM((2, whole, receivers), bf),
            pltpu.VMEM((receivers, 2 * receivers), bf),
            pltpu.VMEM((2, whole, receivers), bf),
            pltpu.SemaphoreType.DMA((2,)),
            pltpu.SemaphoreType.DMA((4,)),
            pltpu.SemaphoreType.DMA((n,)),
            pltpu.SemaphoreType.DMA((2,)),
            pltpu.SemaphoreType.DMA,
        ],
        compiler_params=pltpu.CompilerParams(
            collective_id=0, has_side_effects=True, vmem_limit_bytes=67000000,
        ),
        name="exchange",
    )(primary_one, primary_two, primary_three, window_start, window_end, table)
    return pl.pallas_call(
        inverse_kernel,
        out_shape=jax.ShapeDtypeStruct(primary_one.shape, bf),
        grid=(sources // sub,),
        in_specs=[vmem, vmem],
        out_specs=pl.BlockSpec((sub, receivers, samples), lambda i: (i, 0, 0)),
        scratch_shapes=[pltpu.VMEM((GROUP, 2 * count, receivers), jnp.float32)],
        name="inverse",
    )(piece, table)


def solution(mesh):
    return jax.shard_map(
        on_device,
        mesh=mesh,
        in_specs=(
            P(("groups", "freq"), None, None),
            P(("groups", "freq"), None, None),
            P(("groups", "freq"), None, None),
            P(None, ("groups", "freq"), None),
            P(None, ("groups", "freq"), None),
        ),
        out_specs=P(("groups", "freq"), None, None),
        check_vma=False,
    )
```
